32 devices in a mesh: kpt: 2 (over x), gx: 16 (over z, y, core).
Axes of the slice: x: 2, y: 2, z: 4, core: 2. Of those that a mesh axis runs over, the one named last changes fastest.
Arguments:
- e_field: float32 [2, 3, 64, 512, 128], P(None, None, ('kpt', 'gx')), parts along dimension 2, may hold values from -6 to 6
- h_field: float32 [2, 3, 64, 512, 128], P(None, None, ('kpt', 'gx')), parts along dimension 2, may hold values from -6 to 6
- labels: int32 [64, 512, 128], P(('kpt', 'gx')), parts along dimension 0, may hold values from 0 to 3
- kpoint: int32 [4], P('kpt'), parts along dimension 0, may hold values from 0 to 15
- eps_inf: float32 [4], replicated, may hold values from 1 to 12
- delta_eps: float32 [4], replicated, may hold values from 0.5 to 4
- omega_zero: float32 [4], replicated, may hold values from 0.2 to 1
- damping: float32 [4], replicated, may hold values from 0.05 to 0.8
Outputs:
- e_final: float32 [2, 3, 64, 512, 128], P(None, None, ('kpt', 'gx')), parts along dimension 2
- h_final: float32 [2, 3, 64, 512, 128], P(None, None, ('kpt', 'gx')), parts along dimension 2
The draws below stay inside these ranges and needn't reach their ends.
There are 2 independent parts, one for each index of `kpt`. The reference program is written for one: setup_inputs(seed, part) draws one part's arguments, and reference() takes and returns one part's arrays. A program takes and returns all parts, laid end to end along the dimension named above; an argument that names none is the same for every part. Nothing has to cross between parts.
Inputs may be any that keep to these rules, and one draw needn't show every extreme that they name: `kpoint`: entry 0 indexes the k-point along x, entry 1 along y, out of 16 each.
All inputs are finite; a program needn't handle non-finite values.
Results may differ from the reference program's by a relative error of at most 0.00002.
Values sent between devices are 32-bit elements; how exact they have to be, the bound alone decides.
A program may use at most 128 MiB of HBM per device.

```python
import math
import jax
import jax.numpy as jnp
from jax import lax

NY = 512
NZ = 128
ITERS = 12
LABELS = 4
KGRID = 16
NX = 32


def with_ends(entries, key, least, top_value):
    spot = [jax.random.randint(jax.random.fold_in(key, axis), (), 0, length) for axis, length in enumerate(entries.shape)]
    longest = entries.shape.index(max(entries.shape))
    beside = spot[:longest] + [(spot[longest] + 1) % entries.shape[longest]] + spot[longest + 1:]
    return entries.at[tuple(spot)].set(least).at[tuple(beside)].set(top_value)


def level_of(key, shape, split, smallest, largest):
    def one(dim, parts):
        draws = jax.random.uniform(jax.random.fold_in(jax.random.fold_in(key, 6), dim), (parts,), jnp.float32, smallest / len(split), largest / len(split))
        return jnp.repeat(jnp.exp(draws), shape[dim] // parts).reshape((-1,) + (1,) * (len(shape) - dim - 1))

    factor_of = one(*split[0])
    for cut in split[1:]:
        factor_of = factor_of * one(*cut)
    return factor_of


def noise(stream_key, shape, scale, bound, split=(), held_as=jnp.bfloat16):
    array = jax.random.normal(stream_key, shape, jnp.float32) * scale
    if len(split) > 0:
        array = level_of(stream_key, shape, split, -0.22, 0.18) * array
    return jnp.clip(array, min=-bound, max=bound).astype(held_as)


def setup_inputs(seed: int = 0, part: int = 0) -> dict:
    key_of = jax.random.split(jax.random.key(seed), 9)
    part_splits = jax.random.split(jax.random.fold_in(key_of[8], part), 9)
    return {
        "e_field": noise(part_splits[0], (2, 3, NX, NY, NZ), 1.0, 6.0, ((2, 16),), jnp.float32),
        "h_field": noise(part_splits[1], (2, 3, NX, NY, NZ), 1.0, 6.0, ((2, 16),), jnp.float32),
        "labels": with_ends(jax.random.randint(part_splits[2], (NX, NY, NZ), 0, LABELS), jax.random.fold_in(part_splits[2], 1), 0, LABELS - 1).astype(jnp.int32),
        "kpoint": jax.random.randint(part_splits[3], (2,), 0, KGRID).astype(jnp.int32),
        "eps_inf": jnp.clip(jnp.exp(jax.random.uniform(key_of[4], (LABELS,), jnp.float32, math.log(1.0), math.log(12.0))), 1.0, 12.0),
        "delta_eps": jnp.clip(jnp.exp(jax.random.uniform(key_of[5], (LABELS,), jnp.float32, math.log(0.5), math.log(4.0))), 0.5, 4.0),
        "omega_zero": jnp.clip(jnp.exp(jax.random.uniform(key_of[6], (LABELS,), jnp.float32, math.log(0.2), math.log(1.0))), 0.2, 1.0),
        "damping": jnp.clip(jnp.exp(jax.random.uniform(key_of[7], (LABELS,), jnp.float32, math.log(0.05), math.log(0.8))), 0.05, 0.8),
    }


time_step = 0.5


def cmul(field, cosv, sinv):
    return jnp.stack([field[0] * cosv - field[1] * sinv, field[0] * sinv + field[1] * cosv])


def next_axis(field, axis, cosv, sinv):
    rolled = jnp.roll(field, -1, axis=axis)
    count = field.shape[axis]
    inner = lax.slice_in_dim(rolled, 0, count - 1, axis=axis)
    last = cmul(lax.slice_in_dim(rolled, count - 1, count, axis=axis), cosv, sinv)
    return jnp.concatenate([inner, last], axis=axis)


def prev_axis(field, axis, cosv, sinv):
    rolled = jnp.roll(field, 1, axis=axis)
    count = field.shape[axis]
    first = cmul(lax.slice_in_dim(rolled, 0, 1, axis=axis), cosv, -sinv)
    inner = lax.slice_in_dim(rolled, 1, count, axis=axis)
    return jnp.concatenate([first, inner], axis=axis)


def next_z(field):
    zeros = jnp.zeros(field.shape[:-1] + (1,), jnp.float32)
    return jnp.concatenate([field[..., 1:], zeros], axis=-1)


def prev_z(field):
    zeros = jnp.zeros(field.shape[:-1] + (1,), jnp.float32)
    return jnp.concatenate([zeros, field[..., :-1]], axis=-1)


def per_cell(labels, table):
    picked = jnp.zeros(labels.shape, jnp.float32)
    for label in range(table.shape[0]):
        picked = picked + jnp.where(labels == label, table[label], jnp.float32(0.0))
    return picked


def reference(e_field, h_field, labels, kpoint, eps_inf, delta_eps, omega_zero, damping):
    theta_x = jnp.float32(2.0 * math.pi) * kpoint[0].astype(jnp.float32) / KGRID
    theta_y = jnp.float32(2.0 * math.pi) * kpoint[1].astype(jnp.float32) / KGRID
    cos_x, sin_x = jnp.cos(theta_x), jnp.sin(theta_x)
    cos_y, sin_y = jnp.cos(theta_y), jnp.sin(theta_y)
    half = damping * time_step / 2.0
    ce = per_cell(labels, time_step / eps_inf)
    ja = per_cell(labels, (1.0 - half) / (1.0 + half))
    jb = per_cell(labels, time_step * omega_zero * omega_zero / (1.0 + half))
    de = per_cell(labels, delta_eps)

    def advance(step, carry):
        efield, hfield, polar, current = carry
        ex, ey, ez = efield[:, 0], efield[:, 1], efield[:, 2]
        curl_x = (next_axis(ez, -2, cos_y, sin_y) - ez) - (next_z(ey) - ey)
        curl_y = (next_z(ex) - ex) - (next_axis(ez, -3, cos_x, sin_x) - ez)
        curl_z = (next_axis(ey, -3, cos_x, sin_x) - ey) - (next_axis(ex, -2, cos_y, sin_y) - ex)
        hfield = hfield - time_step * jnp.stack([curl_x, curl_y, curl_z], axis=1)
        hx, hy, hz = hfield[:, 0], hfield[:, 1], hfield[:, 2]
        kurl_x = (hz - prev_axis(hz, -2, cos_y, sin_y)) - (hy - prev_z(hy))
        kurl_y = (hx - prev_z(hx)) - (hz - prev_axis(hz, -3, cos_x, sin_x))
        kurl_z = (hy - prev_axis(hy, -3, cos_x, sin_x)) - (hx - prev_axis(hx, -2, cos_y, sin_y))
        kurl = jnp.stack([kurl_x, kurl_y, kurl_z], axis=1)
        current = ja * current + jb * (de * efield - polar)
        polar = polar + time_step * current
        efield = efield + ce * (kurl - current)
        return efield, hfield, polar, current

    zeros = jnp.zeros(e_field.shape, jnp.float32)
    efield, hfield, polar, current = lax.fori_loop(0, ITERS, advance, (e_field, h_field, zeros, zeros))
    return efield, hfield
```

```python
import math

import jax
import jax.numpy as jnp
from jax import lax
from jax.experimental import pallas as pl
from jax.experimental.pallas import tpu as pltpu
from jax.sharding import PartitionSpec as P

ITERS = 12
KGRID = 16
BLOCK = 8
CHUNKS = 7
LAG = 2
UNROLL = 5
LOW = 24
GHOST = 16
BASE = 13

time_step = 0.5


def turned(re, im, cosv, sinv):
    return re * cosv - im * sinv, re * sinv + im * cosv


def chunk_sizes(half):
    blocks = (half + 24) // BLOCK
    return [BLOCK * (blocks // CHUNKS + (c < blocks % CHUNKS)) for c in range(CHUNKS)]


def edges_of(half):
    starts = [0]
    for size in chunk_sizes(half):
        starts.append(starts[-1] + size)
    return starts


def pieces_in(half):
    starts = edges_of(half)
    pieces = []
    for c in range(CHUNKS):
        lo = starts[c] + 16 if c else LOW - GHOST
        hi = starts[c + 1] + 16
        cuts = [lo] + [k for k in (LOW, LOW + half) if lo < k < hi] + [hi]
        pieces.append(list(zip(cuts[:-1], cuts[1:])))
    return pieces


def pieces_out(half):
    starts = edges_of(half)
    return [(max(starts[c], LOW), min(starts[c + 1], LOW + half)) for c in range(CHUNKS)]


def kernel(e_in, h_in, lab_in, table, phase, e_out, h_out,
           e, h, pol, cur, coef, lab, *scratch):
    stages = [scratch[4 * c:4 * c + 4] for c in range(CHUNKS)]
    in_send, in_recv, se, re, sh, rh, so, ro = scratch[4 * CHUNKS:]
    gx = lax.axis_size("gx")
    me = lax.axis_index("gx")
    q = lax.rem(me, 4)
    base = me - q
    y = lax.div(q, 2)
    core = lax.rem(q, 2)
    left = lax.rem(me + gx - 3 + 2 * core, gx)
    right = lax.rem(me + 1 + 2 * core, gx)
    local, total_rows, width = lab_in.shape
    half = total_rows // 2
    planes = 2 * local
    rows = lab.shape[1]
    starts = edges_of(half)
    sizes = chunk_sizes(half)
    ins, outs = pieces_in(half), pieces_out(half)
    ph = [phase[i] for i in range(8)]
    turn_r, turn_l, turn_low, turn_high = [(ph[2 * i], ph[2 * i + 1]) for i in range(4)]

    def remote(src, dst, send, recv, to):
        return pltpu.make_async_remote_copy(
            src_ref=src, dst_ref=dst, send_sem=send, recv_sem=recv,
            device_id={"gx": to}, device_id_type=pl.DeviceIdType.MESH)

    barrier = pltpu.get_barrier_semaphore()
    others = [base + lax.rem(q + k, 4) for k in (1, 2, 3)]
    others += [lax.rem(me + gx + k, gx) for k in (-3, -1, 1, 3)]
    for other in others:
        pl.semaphore_signal(barrier, inc=1, device_id={"gx": other},
                            device_id_type=pl.DeviceIdType.MESH)
    pl.semaphore_wait(barrier, len(others))

    segments = [(c, seg) for c in range(CHUNKS) for seg in ins[c]]

    def move_in(n, dest, slot):
        lo, hi = segments[n][1]
        first = (dest * half + lo - LOW) % total_rows
        src, dst = pl.ds(first, hi - lo), pl.ds(lo, hi - lo)
        group = pl.ds(slot * local, local)
        return ((lab_in.at[:, src], lab.at[group, dst]),
                (e_in.at[:, :, :, src], e.at[:, :, group, dst]),
                (h_in.at[:, :, :, src], h.at[:, :, group, dst]))

    def each_move_in(n, act):
        for dest in range(2):
            for slot in range(2):
                for k, (src, dst) in enumerate(move_in(n, dest, slot)):
                    away = core == slot
                    if dest == slot:
                        @pl.when((y == dest) & (core == slot))
                        def _():
                            act(None, pltpu.make_async_copy(src, dst, in_recv.at[n, k, slot]))
                        away = away & (y != dest)

                    @pl.when(away)
                    def _():
                        act(remote(src, dst, in_send.at[n, k, dest], in_recv.at[n, k, slot], base + 2 * dest + y), None)

    def start(far, near):
        (far or near).start()

    def sent(far, near):
        if far is not None:
            far.wait_send()

    for n in range(len(segments)):
        each_move_in(n, start)

    def wait_in(n, k):
        for slot in range(2):
            src, dst = move_in(n, 0, slot)[k]
            remote(src, dst, in_send.at[n, k, 0], in_recv.at[n, k, slot], base + lax.rem(q + 1, 4)).wait_recv()

    def move_out(c, k, i):
        lo, hi = outs[c]
        ref, out = ((e, e_out), (h, h_out))[k]
        src = ref.at[:, :, pl.ds(i * local, local), pl.ds(lo, hi - lo)]
        to = pl.multiple_of(y * half + (lo - LOW), BLOCK)
        return src, out.at[:, :, :, pl.ds(to, hi - lo)]

    def each_move_out(c, act):
        for k in range(2):
            for i in range(2):
                src, dst = move_out(c, k, i)
                here = (core == i) & (y == i)

                @pl.when(here)
                def _():
                    act(None, pltpu.make_async_copy(src, dst, ro.at[c, k, i]))

                @pl.when(jnp.logical_not(here))
                def _():
                    act(remote(src, dst, so.at[c, k, i], ro.at[c, k, y], base + 2 * core + i), None)

    def wait_out(c):
        for k in range(2):
            for other in range(2):
                src, dst = move_out(c, k, 0)
                remote(src, dst, so.at[c, k, 0], ro.at[c, k, other], base + lax.rem(q + 1, 4)).wait_recv()

    def send_e(c, par):
        return remote(stages[c][0], stages[c][2].at[par], se.at[c], re.at[c, par], left)

    def send_h(c, par):
        return remote(stages[c][1], stages[c][3].at[par], sh.at[c], rh.at[c, par], right)

    lane = lax.broadcasted_iota(jnp.int32, (BLOCK, width), 1)
    not_end = lane < width - 1
    not_start = lane > 0
    zero = jnp.zeros((BLOCK, width), jnp.float32)

    def next_z(f):
        return jnp.where(not_end, pltpu.roll(f, width - 1, 1), 0.0)

    def prev_z(f):
        return jnp.where(not_start, pltpu.roll(f, 1, 1), 0.0)

    @pl.loop(0, rows // BLOCK)
    def _(i):
        here = pl.ds(pl.multiple_of(i * BLOCK, BLOCK), BLOCK)
        for x in range(planes):
            for ri in range(2):
                for a in range(3):
                    pol[ri, a, x, here] = zero
                    cur[ri, a, x, here] = zero

    for x in range(planes):
        for which in range(4):
            coef[which, x, 0:BLOCK] = zero
        for ri in range(2):
            for a in range(3):
                e[ri, a, x, 0:BLOCK] = zero
                h[ri, a, x, 0:BLOCK] = zero

    def fill_coef(lo, hi):
        @pl.loop(0, (hi - lo) // BLOCK)
        def _(i):
            here = pl.ds(pl.multiple_of(lo + i * BLOCK, BLOCK), BLOCK)
            for x in range(planes):
                label = lab[x, here]
                masks = [label == k for k in range(table.shape[1])]
                for which in range(4):
                    picked = zero
                    for k, mask in enumerate(masks):
                        picked = picked + jnp.where(mask, table[which, k], jnp.float32(0.0))
                    coef[which, x, here] = picked

    def turn_rows(ref, lo, hi, turn):
        @pl.loop(0, (hi - lo) // BLOCK)
        def _(i):
            here = pl.ds(pl.multiple_of(lo + i * BLOCK, BLOCK), BLOCK)
            for x in range(planes):
                for a in range(3):
                    re_new, im_new = turned(ref[0, a, x, here], ref[1, a, x, here], *turn)
                    ref[0, a, x, here] = re_new
                    ref[1, a, x, here] = im_new

    def prepare(c, t):
        stage_e, stage_h = stages[c][:2]
        last = planes - 1

        def one(i, carry):
            at = BASE + starts[c] - t + i * BLOCK
            here, up = pl.ds(at, BLOCK), pl.ds(at + 1, BLOCK)
            to = pl.ds(pl.multiple_of(i * BLOCK, BLOCK), BLOCK)
            for ri in range(2):
                stage_e[ri, 0, to] = e[ri, 1, 0, here]
                stage_e[ri, 1, to] = e[ri, 2, 0, here]
                ex, ey, ez = [e[ri, a, last, here] for a in range(3)]
                hy = h[ri, 1, last, here] - time_step * ((next_z(ex) - ex) + ez)
                hz = h[ri, 2, last, here] + time_step * (ey + (e[ri, 0, last, up] - ex))
                h[ri, 1, last, here] = hy
                h[ri, 2, last, here] = hz
                stage_h[ri, 0, to] = hy
                stage_h[ri, 1, to] = hz
            return carry
        lax.fori_loop(0, sizes[c] // BLOCK, one, 0, unroll=UNROLL)
        par = lax.rem(t, 2)
        send_h(c, par).start()
        send_e(c, par).start()

    def advance(c, t):
        par = lax.rem(t, 2)
        send_h(c, par).wait_recv()
        send_e(c, par).wait_recv()
        ge, gh = stages[c][2].at[par], stages[c][3].at[par]

        def one(i, carry):
            at = BASE + starts[c] - t + i * BLOCK
            here, up, down = pl.ds(at, BLOCK), pl.ds(at + 1, BLOCK), pl.ds(at - 1, BLOCK)
            to = pl.ds(pl.multiple_of(i * BLOCK, BLOCK), BLOCK)
            field = [[e[ri, a, 0, here] for a in range(3)] for ri in range(2)]
            before = [turned(gh[0, a, to], gh[1, a, to], *turn_l) for a in range(2)]
            prev_y = [before[0][ri] + time_step * field[ri][2] for ri in range(2)]
            prev_zz = [before[1][ri] - time_step * field[ri][1] for ri in range(2)]
            for x in range(planes):
                at_last = x == planes - 1
                if at_last:
                    beyond = [turned(ge[0, a, to], ge[1, a, to], *turn_r) for a in range(2)]
                else:
                    later = [[e[ri, a, x + 1, here] for a in range(3)] for ri in range(2)]
                new = []
                for ri in range(2):
                    ex, ey, ez = field[ri]
                    hx = h[ri, 0, x, here] - time_step * ((e[ri, 2, x, up] - ez) - (next_z(ey) - ey))
                    if at_last:
                        hy = h[ri, 1, x, here] + time_step * beyond[1][ri]
                        hz = h[ri, 2, x, here] - time_step * beyond[0][ri]
                    else:
                        hy = h[ri, 1, x, here] - time_step * ((next_z(ex) - ex) - (later[ri][2] - ez))
                        hz = h[ri, 2, x, here] - time_step * ((later[ri][1] - ey) - (e[ri, 0, x, up] - ex))
                    h[ri, 0, x, here] = hx
                    h[ri, 1, x, here] = hy
                    h[ri, 2, x, here] = hz
                    new.append((hx, hy, hz))
                ce, ja, jb, de = [coef[k, x, here] for k in range(4)]
                for ri in range(2):
                    hx, hy, hz = new[ri]
                    kx = (hz - h[ri, 2, x, down]) - (hy - prev_z(hy))
                    ky = (hx - prev_z(hx)) - (hz - prev_zz[ri])
                    kz = (hy - prev_y[ri]) - (hx - h[ri, 0, x, down])
                    for a, kurl in enumerate((kx, ky, kz)):
                        polar = pol[ri, a, x, here]
                        current = ja * cur[ri, a, x, here] + jb * (de * field[ri][a] - polar)
                        cur[ri, a, x, here] = current
                        pol[ri, a, x, here] = polar + time_step * current
                        e[ri, a, x, here] = field[ri][a] + ce * (kurl - current)
                    prev_y[ri], prev_zz[ri] = hy, hz
                if not at_last:
                    field = later
            return carry
        lax.fori_loop(0, sizes[c] // BLOCK, one, 0, unroll=1)

    def arrive(c):
        mine = [n for n, (chunk, _) in enumerate(segments) if chunk == c]
        for n in mine:
            wait_in(n, 0)
        for n in mine:
            lo, hi = segments[n][1]
            fill_coef(lo, hi)
        for n in mine:
            lo, hi = segments[n][1]
            for k, ref in ((1, e), (2, h)):
                wait_in(n, k)
                if hi <= LOW:
                    turn_rows(ref, lo, hi, turn_low)
                if lo >= LOW + half:
                    turn_rows(ref, lo, hi, turn_high)
        prepare(c, 1)

    waves = LAG * (CHUNKS - 1) + ITERS + 1

    @pl.loop(0, waves)
    def _(w):
        for c in range(CHUNKS):
            t = w - LAG * c

            @pl.when((t >= 1) & (t <= ITERS))
            def _():
                advance(c, t)
                send_h(c, 0).wait_send()
                send_e(c, 0).wait_send()

                @pl.when(t < ITERS)
                def _():
                    prepare(c, t + 1)

                @pl.when(t == ITERS)
                def _():
                    each_move_out(c, start)

        for c in range(CHUNKS):
            @pl.when(w == LAG * c)
            def _():
                arrive(c)

    for n in range(len(segments)):
        each_move_in(n, sent)
    for c in range(CHUNKS):
        each_move_out(c, sent)
        wait_out(c)


def shards(e_field, h_field, labels, kpoint, eps_inf, delta_eps, omega_zero, damping):
    theta_x = jnp.float32(2.0 * math.pi) * kpoint[0].astype(jnp.float32) / KGRID
    theta_y = jnp.float32(2.0 * math.pi) * kpoint[1].astype(jnp.float32) / KGRID
    cos_x, sin_x = (jnp.cos(theta_x), jnp.sin(theta_x))
    cos_y, sin_y = (jnp.cos(theta_y), jnp.sin(theta_y))
    damped = damping * time_step / 2.0
    table = jnp.stack([
        time_step / eps_inf,
        (1.0 - damped) / (1.0 + damped),
        time_step * omega_zero * omega_zero / (1.0 + damped),
        delta_eps,
    ])
    position = lax.axis_index("gx")
    size = lax.axis_size("gx")
    one, nought = jnp.float32(1.0), jnp.float32(0.0)
    y = lax.rem(lax.div(position, 2), 2)
    first = (position < 4) & (lax.rem(position, 2) == 0)
    last = (position >= size - 4) & (lax.rem(position, 2) == 1)

    def turn(where, cosv, sinv):
        return [jnp.where(where, cosv, one), jnp.where(where, sinv, nought)]

    phase = jnp.stack(
        turn(last, cos_x, sin_x) + turn(first, cos_x, -sin_x)
        + turn(y == 0, cos_y, -sin_y) + turn(y == 1, cos_y, sin_y))
    local, total_rows, width = labels.shape
    half = total_rows // 2
    planes = 2 * local
    rows = half + LOW + GHOST
    state = (2, 3, local, total_rows, width)
    field = (2, 3, planes, rows, width)
    count = sum(len(p) for p in pieces_in(half))
    dma = pltpu.SemaphoreType.DMA
    anywhere = pl.BlockSpec(memory_space=pl.ANY)
    scalars = pl.BlockSpec(memory_space=pltpu.SMEM)
    halos = []
    for size in chunk_sizes(half):
        halos += [pltpu.VMEM((2, 2, size, width), jnp.float32)] * 2
        halos += [pltpu.VMEM((2, 2, 2, size, width), jnp.float32)] * 2
    return pl.pallas_call(
        kernel,
        out_shape=(jax.ShapeDtypeStruct(state, jnp.float32),) * 2,
        in_specs=[anywhere] * 3 + [scalars] * 2,
        out_specs=(anywhere, anywhere),
        scratch_shapes=[pltpu.VMEM(field, jnp.float32)] * 4
        + [pltpu.VMEM((4, planes, rows, width), jnp.float32), pltpu.VMEM((planes, rows, width), jnp.int32)]
        + halos
        + [dma((count, 3, 2)), dma((count, 3, 2)), dma((CHUNKS,)), dma((CHUNKS, 2)),
           dma((CHUNKS,)), dma((CHUNKS, 2)), dma((CHUNKS, 2, 2)), dma((CHUNKS, 2, 2))],
        compiler_params=pltpu.CompilerParams(collective_id=0, has_side_effects=True),
    )(e_field, h_field, labels, table, phase)


def solution(mesh):
    placed = (
        P(None, None, ("kpt", "gx"), None, None),
        P(None, None, ("kpt", "gx"), None, None),
        P(("kpt", "gx"), None, None),
        P("kpt"),
        P(),
        P(),
        P(),
        P(),
    )
    return jax.shard_map(
        shards,
        mesh=mesh,
        in_specs=placed,
        out_specs=(
            P(None, None, ("kpt", "gx"), None, None),
            P(None, None, ("kpt", "gx"), None, None),
        ),
        check_vma=False,
    )
```

```python
import math

import jax
import jax.numpy as jnp
from jax import lax
from jax.experimental import pallas as pl
from jax.experimental.pallas import tpu as pltpu
from jax.sharding import PartitionSpec as P

ITERS = 12
KGRID = 16
BLOCK = 8
SHARES = (3, 3, 3, 3, 3, 3, 3, 3, 3, 3, 3, 2)
BEGIN = (0, 1, 3, 4, 6, 7, 9, 10, 12, 13, 15, 16)
CHUNKS = len(SHARES)
UNROLL_P = 3
UNROLL_H = 3
UNROLL_E = 3
LOW = 24
GHOST = 16
BASE = 13

time_step = 0.5


def turned(re, im, cosv, sinv):
    return re * cosv - im * sinv, re * sinv + im * cosv


def chunk_sizes(half):
    blocks = (half + 24) // BLOCK
    ends = [blocks * sum(SHARES[:c]) // sum(SHARES) for c in range(CHUNKS + 1)]
    return [BLOCK * (ends[c + 1] - ends[c]) for c in range(CHUNKS)]


def edges_of(half):
    starts = [0]
    for size in chunk_sizes(half):
        starts.append(starts[-1] + size)
    return starts


def pieces_in(half):
    starts = edges_of(half)
    pieces = []
    for c in range(CHUNKS):
        lo = starts[c] + 16 if c else LOW - GHOST
        hi = starts[c + 1] + 16
        cuts = [lo] + [k for k in (LOW, LOW + half) if lo < k < hi] + [hi]
        pieces.append(list(zip(cuts[:-1], cuts[1:])))
    return pieces


def pieces_out(half):
    starts = edges_of(half)
    return [(max(starts[c], LOW), min(starts[c + 1], LOW + half)) for c in range(CHUNKS)]


def kernel(e_in, h_in, lab_in, kpoint, eps_inf, delta_eps, omega_zero, damping, e_out, h_out,
           e, h, pol, cur, coef, lab, table, phase, *scratch):
    stages = [scratch[4 * c:4 * c + 4] for c in range(CHUNKS)]
    in_send, in_recv, se, re, sh, rh, so, ro = scratch[4 * CHUNKS:]
    gx = lax.axis_size("gx")
    me = lax.axis_index("gx")
    q = lax.rem(me, 4)
    base = me - q
    y = lax.div(q, 2)
    core = lax.rem(q, 2)
    left = lax.rem(me + gx - 3 + 2 * core, gx)
    right = lax.rem(me + 1 + 2 * core, gx)
    local, total_rows, width = lab_in.shape
    half = total_rows // 2
    planes = 2 * local
    rows = lab.shape[1]
    starts = edges_of(half)
    sizes = chunk_sizes(half)
    ins, outs = pieces_in(half), pieces_out(half)
    labels = eps_inf.shape[0]

    def turn_of(i):
        return phase[2 * i], phase[2 * i + 1]

    def remote(src, dst, send, recv, to):
        return pltpu.make_async_remote_copy(
            src_ref=src, dst_ref=dst, send_sem=send, recv_sem=recv,
            device_id={"gx": to}, device_id_type=pl.DeviceIdType.MESH)

    barrier = pltpu.get_barrier_semaphore()
    others = [base + lax.rem(q + k, 4) for k in (1, 2, 3)]
    others += [lax.rem(me + gx + k, gx) for k in (-3, -1, 1, 3)]
    for other in others:
        pl.semaphore_signal(barrier, inc=1, device_id={"gx": other},
                            device_id_type=pl.DeviceIdType.MESH)
    pl.semaphore_wait(barrier, len(others))

    segments = [(c, seg) for c in range(CHUNKS) for seg in ins[c]]

    def move_in(n, dest, slot):
        lo, hi = segments[n][1]
        first = (dest * half + lo - LOW) % total_rows
        src, dst = pl.ds(first, hi - lo), pl.ds(lo, hi - lo)
        group = pl.ds(slot * local, local)
        return ((lab_in.at[:, src], lab.at[group, dst]),
                (e_in.at[:, :, :, src], e.at[:, :, group, dst]),
                (h_in.at[:, :, :, src], h.at[:, :, group, dst]))

    def each_move_in(n, act):
        for dest in range(2):
            for slot in range(2):
                for k, (src, dst) in enumerate(move_in(n, dest, slot)):
                    away = core == slot
                    if dest == slot:
                        @pl.when((y == dest) & (core == slot))
                        def _():
                            act(None, pltpu.make_async_copy(src, dst, in_recv.at[n, k, slot]))
                        away = away & (y != dest)

                    @pl.when(away)
                    def _():
                        act(remote(src, dst, in_send.at[n, k, dest], in_recv.at[n, k, slot], base + 2 * dest + y), None)

    def start(far, near):
        (far or near).start()

    def sent(far, near):
        if far is not None:
            far.wait_send()

    for n in range(len(segments)):
        each_move_in(n, start)

    def spread(value):
        return jnp.full((BLOCK, width), value, jnp.float32)

    for k in range(labels):
        damped = spread(damping[k]) * time_step / 2.0
        omega = spread(omega_zero[k])
        table[k] = time_step / spread(eps_inf[k])
        table[labels + k] = (1.0 - damped) / (1.0 + damped)
        table[2 * labels + k] = time_step * omega * omega / (1.0 + damped)
        table[3 * labels + k] = spread(delta_eps[k])

    cos_sin = []
    for axis in range(2):
        theta = spread(2.0 * math.pi) * spread(kpoint[axis].astype(jnp.float32)) / KGRID
        cos_sin.append((jnp.cos(theta), jnp.sin(theta)))
    (cos_x, sin_x), (cos_y, sin_y) = cos_sin
    turns = (((me >= gx - 4) & (core == 1), cos_x, sin_x), ((me < 4) & (core == 0), cos_x, -sin_x),
             (y == 0, cos_y, -sin_y), (y == 1, cos_y, sin_y))
    for i, (where, cosv, sinv) in enumerate(turns):
        phase[2 * i] = jnp.where(where, cosv, 1.0)
        phase[2 * i + 1] = jnp.where(where, sinv, 0.0)

    def wait_in(n, k):
        for slot in range(2):
            src, dst = move_in(n, 0, slot)[k]
            remote(src, dst, in_send.at[n, k, 0], in_recv.at[n, k, slot], base + lax.rem(q + 1, 4)).wait_recv()

    def move_out(c, k, i):
        lo, hi = outs[c]
        ref, out = ((e, e_out), (h, h_out))[k]
        src = ref.at[:, :, pl.ds(i * local, local), pl.ds(lo, hi - lo)]
        to = pl.multiple_of(y * half + (lo - LOW), BLOCK)
        return src, out.at[:, :, :, pl.ds(to, hi - lo)]

    def each_move_out(c, act):
        for k in range(2):
            for i in range(2):
                src, dst = move_out(c, k, i)
                here = (core == i) & (y == i)

                @pl.when(here)
                def _():
                    act(None, pltpu.make_async_copy(src, dst, ro.at[c, k, i]))

                @pl.when(jnp.logical_not(here))
                def _():
                    act(remote(src, dst, so.at[c, k, i], ro.at[c, k, y], base + 2 * core + i), None)

    def wait_out(c):
        for k in range(2):
            for other in range(2):
                src, dst = move_out(c, k, 0)
                remote(src, dst, so.at[c, k, 0], ro.at[c, k, other], base + lax.rem(q + 1, 4)).wait_recv()

    def halos(c, t, act):
        par = lax.rem(t, 2)

        def both(cut):
            kept = pl.ds(cut, sizes[c] - cut)
            for k, (send, recv, to) in enumerate(((se, re, left), (sh, rh, right))):
                act(remote(stages[c][k].at[:, :, kept], stages[c][2 + k].at[par, :, :, kept],
                           send.at[c], recv.at[c, par], to))

        if c:
            both(0)
        else:
            for k in range((ITERS - 1) // 4 + 1):
                @pl.when(lax.div(t - 1, 4) == k)
                def _():
                    both(BLOCK * k)

    def block_loop(c, t, body, unroll):
        count = sizes[c] // BLOCK
        first = 0
        if not c:
            first = (ITERS - 1) // 4
            for i in range(first):
                @pl.when(lax.div(t - 1, 4) <= i)
                def _():
                    body(i, 0)
        left_over = count - first
        lax.fori_loop(first, count, body, 0, unroll=unroll if left_over % unroll == 0 else 1)

    lane = lax.broadcasted_iota(jnp.int32, (BLOCK, width), 1)
    not_end = lane < width - 1
    not_start = lane > 0
    zero = jnp.zeros((BLOCK, width), jnp.float32)

    def rows_at(i):
        return pl.ds(i * BLOCK if isinstance(i, int) else pl.multiple_of(i * BLOCK, BLOCK), BLOCK)

    def next_z(f):
        return jnp.where(not_end, pltpu.roll(f, width - 1, 1), 0.0)

    def prev_z(f):
        return jnp.where(not_start, pltpu.roll(f, 1, 1), 0.0)

    @pl.loop(0, rows // BLOCK)
    def _(i):
        here = pl.ds(pl.multiple_of(i * BLOCK, BLOCK), BLOCK)
        for x in range(planes):
            for ri in range(2):
                for a in range(3):
                    pol[ri, a, x, here] = zero
                    cur[ri, a, x, here] = zero

    for x in range(planes):
        for which in range(4):
            coef[which, x, 0:BLOCK] = zero
        for ri in range(2):
            for a in range(3):
                e[ri, a, x, 0:BLOCK] = zero
                h[ri, a, x, 0:BLOCK] = zero

    def fill_coef(lo, hi):
        @pl.loop(0, (hi - lo) // BLOCK)
        def _(i):
            here = pl.ds(pl.multiple_of(lo + i * BLOCK, BLOCK), BLOCK)
            for x in range(planes):
                label = lab[x, here]
                masks = [label == k for k in range(labels)]
                for which in range(4):
                    picked = zero
                    for k, mask in enumerate(masks):
                        picked = picked + jnp.where(mask, table[which * labels + k], 0.0)
                    coef[which, x, here] = picked

    def turn_rows(ref, lo, hi, turn):
        @pl.loop(0, (hi - lo) // BLOCK)
        def _(i):
            here = pl.ds(pl.multiple_of(lo + i * BLOCK, BLOCK), BLOCK)
            for x in range(planes):
                for a in range(3):
                    re_new, im_new = turned(ref[0, a, x, here], ref[1, a, x, here], *turn)
                    ref[0, a, x, here] = re_new
                    ref[1, a, x, here] = im_new

    last = planes - 1

    def spots(c, t, i):
        at = BASE + starts[c] - t + i * BLOCK
        return [pl.ds(at + k, BLOCK) for k in (-1, 0, 1)] + [rows_at(i)]

    def prepare(c, t):
        stage_e, stage_h = stages[c][:2]

        def one(i, carry):
            down, here, up, to = spots(c, t, i)
            for ri in range(2):
                stage_e[ri, 0, to] = e[ri, 1, 0, here]
                stage_e[ri, 1, to] = e[ri, 2, 0, here]
                ex, ey, ez = [e[ri, a, last, here] for a in range(3)]
                hy = h[ri, 1, last, here] - time_step * ((next_z(ex) - ex) + ez)
                hz = h[ri, 2, last, here] + time_step * (ey + (e[ri, 0, last, up] - ex))
                h[ri, 1, last, here] = hy
                h[ri, 2, last, here] = hz
                stage_h[ri, 0, to] = hy
                stage_h[ri, 1, to] = hz
            return carry
        block_loop(c, t, one, UNROLL_P)
        halos(c, t, lambda copy: copy.start())

    def inner(c, t):
        def one(i, carry):
            down, here, up, to = spots(c, t, i)
            field = [[e[ri, a, 0, here] for a in range(3)] for ri in range(2)]
            for x in range(planes):
                if x < last:
                    later = [[e[ri, a, x + 1, here] for a in range(3)] for ri in range(2)]
                for ri in range(2):
                    ex, ey, ez = field[ri]
                    h[ri, 0, x, here] = h[ri, 0, x, here] - time_step * ((e[ri, 2, x, up] - ez) - (next_z(ey) - ey))
                    if x < last:
                        h[ri, 1, x, here] = h[ri, 1, x, here] - time_step * ((next_z(ex) - ex) - (later[ri][2] - ez))
                        h[ri, 2, x, here] = h[ri, 2, x, here] - time_step * ((later[ri][1] - ey) - (e[ri, 0, x, up] - ex))
                field = later
            return carry
        block_loop(c, t, one, UNROLL_H)

    def complete(c, t):
        ge = stages[c][2].at[lax.rem(t, 2)]

        def one(i, carry):
            down, here, up, to = spots(c, t, i)
            beyond = [turned(ge[0, a, to], ge[1, a, to], *turn_of(0)) for a in range(2)]
            for ri in range(2):
                h[ri, 1, last, here] = h[ri, 1, last, here] + time_step * beyond[1][ri]
                h[ri, 2, last, here] = h[ri, 2, last, here] - time_step * beyond[0][ri]
            return carry
        block_loop(c, t, one, UNROLL_P)

    def electric(c, t, order):
        gh = stages[c][3].at[lax.rem(t, 2)]

        def one(i, carry):
            down, here, up, to = spots(c, t, i)
            for x in order:
                if x:
                    prev_y, prev_zz = [[h[ri, a, x - 1, here] for ri in range(2)] for a in (1, 2)]
                else:
                    before = [turned(gh[0, a, to], gh[1, a, to], *turn_of(1)) for a in range(2)]
                    prev_y = [before[0][ri] + time_step * e[ri, 2, 0, here] for ri in range(2)]
                    prev_zz = [before[1][ri] - time_step * e[ri, 1, 0, here] for ri in range(2)]
                ce, ja, jb, de = [coef[k, x, here] for k in range(4)]
                for ri in range(2):
                    hx, hy, hz = [h[ri, a, x, here] for a in range(3)]
                    kx = (hz - h[ri, 2, x, down]) - (hy - prev_z(hy))
                    ky = (hx - prev_z(hx)) - (hz - prev_zz[ri])
                    kz = (hy - prev_y[ri]) - (hx - h[ri, 0, x, down])
                    for a, kurl in enumerate((kx, ky, kz)):
                        field, polar = e[ri, a, x, here], pol[ri, a, x, here]
                        current = ja * cur[ri, a, x, here] + jb * (de * field - polar)
                        cur[ri, a, x, here] = current
                        pol[ri, a, x, here] = polar + time_step * current
                        e[ri, a, x, here] = field + ce * (kurl - current)
            return carry
        block_loop(c, t, one, UNROLL_E)

    def advance(c, t):
        halos(c, t, lambda copy: copy.wait_recv())
        complete(c, t)
        electric(c, t, (0, last))
        halos(c, t, lambda copy: copy.wait_send())

        @pl.when(t < ITERS)
        def _():
            prepare(c, t + 1)
        electric(c, t, range(1, last))

        @pl.when(t < ITERS)
        def _():
            inner(c, t + 1)

        @pl.when(t == ITERS)
        def _():
            each_move_out(c, start)

    def arrive(c):
        mine = [n for n, (chunk, _) in enumerate(segments) if chunk == c]
        for n in mine:
            wait_in(n, 0)
        for n in mine:
            lo, hi = segments[n][1]
            fill_coef(lo, hi)
        for n in mine:
            lo, hi = segments[n][1]
            for k, ref in ((1, e), (2, h)):
                wait_in(n, k)
                if hi <= LOW:
                    turn_rows(ref, lo, hi, turn_of(2))
                if lo >= LOW + half:
                    turn_rows(ref, lo, hi, turn_of(3))
        prepare(c, 1)
        inner(c, 1)

    waves = BEGIN[-1] + ITERS + 1

    @pl.loop(0, waves)
    def _(w):
        for c in range(CHUNKS):
            t = w - BEGIN[c]

            @pl.when((t >= 1) & (t <= ITERS))
            def _():
                advance(c, t)

        for c in range(CHUNKS):
            @pl.when(w == BEGIN[c])
            def _():
                arrive(c)

    for n in range(len(segments)):
        each_move_in(n, sent)
    for c in range(CHUNKS):
        each_move_out(c, sent)
        wait_out(c)


def shards(e_field, h_field, labels, kpoint, eps_inf, delta_eps, omega_zero, damping):
    local, total_rows, width = labels.shape
    half = total_rows // 2
    planes = 2 * local
    rows = half + LOW + GHOST
    state = (2, 3, local, total_rows, width)
    field = (2, 3, planes, rows, width)
    count = sum(len(p) for p in pieces_in(half))
    dma = pltpu.SemaphoreType.DMA
    anywhere = pl.BlockSpec(memory_space=pl.ANY)
    scalars = pl.BlockSpec(memory_space=pltpu.SMEM)
    halos = []
    for size in chunk_sizes(half):
        halos += [pltpu.VMEM((2, 2, size, width), jnp.float32)] * 2
        halos += [pltpu.VMEM((2, 2, 2, size, width), jnp.float32)] * 2
    return pl.pallas_call(
        kernel,
        out_shape=(jax.ShapeDtypeStruct(state, jnp.float32),) * 2,
        in_specs=[anywhere] * 3 + [scalars] * 5,
        out_specs=(anywhere, anywhere),
        scratch_shapes=[pltpu.VMEM(field, jnp.float32)] * 4
        + [pltpu.VMEM((4, planes, rows, width), jnp.float32), pltpu.VMEM((planes, rows, width), jnp.int32),
           pltpu.VMEM((4 * eps_inf.shape[0], BLOCK, width), jnp.float32), pltpu.VMEM((8, BLOCK, width), jnp.float32)]
        + halos
        + [dma((count, 3, 2)), dma((count, 3, 2)), dma((CHUNKS,)), dma((CHUNKS, 2)),
           dma((CHUNKS,)), dma((CHUNKS, 2)), dma((CHUNKS, 2, 2)), dma((CHUNKS, 2, 2))],
        compiler_params=pltpu.CompilerParams(collective_id=0, has_side_effects=True),
    )(e_field, h_field, labels, kpoint, eps_inf, delta_eps, omega_zero, damping)


def solution(mesh):
    placed = (
        P(None, None, ("kpt", "gx"), None, None),
        P(None, None, ("kpt", "gx"), None, None),
        P(("kpt", "gx"), None, None),
        P("kpt"),
        P(),
        P(),
        P(),
        P(),
    )
    return jax.shard_map(
        shards,
        mesh=mesh,
        in_specs=placed,
        out_specs=(
            P(None, None, ("kpt", "gx"), None, None),
            P(None, None, ("kpt", "gx"), None, None),
        ),
        check_vma=False,
    )
```

```python
import math

import jax
import jax.numpy as jnp
from jax import lax
from jax.experimental import pallas as pl
from jax.experimental.pallas import tpu as pltpu
from jax.sharding import PartitionSpec as P

ITERS = 12
KGRID = 16
BLOCK = 8
SHARES = (3, 2, 2, 2, 2, 2, 2, 2, 2, 2, 2, 2, 2, 2, 2, 2, 2)
BEGIN = (0, 1, 2, 3, 4, 5, 6, 7, 8, 9, 10, 11, 12, 13, 14, 15, 16)
CHUNKS = len(SHARES)
UNROLL_P = 2
UNROLL_H = 2
UNROLL_E = 2
LOW = 24
GHOST = 16
BASE = 13

time_step = 0.5


def turned(re, im, cosv, sinv):
    return re * cosv - im * sinv, re * sinv + im * cosv


def chunk_sizes(half):
    blocks = (half + 24) // BLOCK
    ends = [blocks * sum(SHARES[:c]) // sum(SHARES) for c in range(CHUNKS + 1)]
    return [BLOCK * (ends[c + 1] - ends[c]) for c in range(CHUNKS)]


def edges_of(half):
    starts = [0]
    for size in chunk_sizes(half):
        starts.append(starts[-1] + size)
    return starts


def pieces_in(half):
    starts = edges_of(half)
    pieces = []
    for c in range(CHUNKS):
        lo = starts[c] + 16 if c else LOW - GHOST
        hi = starts[c + 1] + 16
        cuts = [lo] + [k for k in (LOW, LOW + half) if lo < k < hi] + [hi]
        pieces.append(list(zip(cuts[:-1], cuts[1:])))
    return pieces


def pieces_out(half):
    starts = edges_of(half)
    return [(max(starts[c], LOW), min(starts[c + 1], LOW + half)) for c in range(CHUNKS)]


def kernel(e_in, h_in, lab_in, kpoint, eps_inf, delta_eps, omega_zero, damping, e_out, h_out,
           e, h, pol, cur, coef, lab, table, phase, *scratch):
    stages = [scratch[4 * c:4 * c + 4] for c in range(CHUNKS)]
    in_send, in_recv, se, re, sh, rh, so, ro = scratch[4 * CHUNKS:]
    gx = lax.axis_size("gx")
    me = lax.axis_index("gx")
    q = lax.rem(me, 4)
    base = me - q
    y = lax.div(q, 2)
    core = lax.rem(q, 2)
    left = lax.rem(me + gx - 3 + 2 * core, gx)
    right = lax.rem(me + 1 + 2 * core, gx)
    local, total_rows, width = lab_in.shape
    half = total_rows // 2
    planes = 2 * local
    rows = lab.shape[1]
    starts = edges_of(half)
    sizes = chunk_sizes(half)
    ins, outs = pieces_in(half), pieces_out(half)
    labels = eps_inf.shape[0]

    def turn_of(i):
        return phase[2 * i], phase[2 * i + 1]

    def remote(src, dst, send, recv, to):
        return pltpu.make_async_remote_copy(
            src_ref=src, dst_ref=dst, send_sem=send, recv_sem=recv,
            device_id={"gx": to}, device_id_type=pl.DeviceIdType.MESH)

    barrier = pltpu.get_barrier_semaphore()
    others = [base + lax.rem(q + k, 4) for k in (1, 2, 3)]
    others += [lax.rem(me + gx + k, gx) for k in (-3, -1, 1, 3)]
    for other in others:
        pl.semaphore_signal(barrier, inc=1, device_id={"gx": other},
                            device_id_type=pl.DeviceIdType.MESH)
    pl.semaphore_wait(barrier, len(others))

    segments = [(c, seg) for c in range(CHUNKS) for seg in ins[c]]

    def move_in(n, dest, slot):
        lo, hi = segments[n][1]
        first = (dest * half + lo - LOW) % total_rows
        src, dst = pl.ds(first, hi - lo), pl.ds(lo, hi - lo)
        group = pl.ds(slot * local, local)
        return ((e_in.at[:, :, :, src], e.at[:, :, group, dst]),
                (h_in.at[:, :, :, src], h.at[:, :, group, dst]),
                (lab_in.at[:, src], lab.at[group, dst]))

    def each_move_in(n, act):
        for dest in range(2):
            for slot in range(2):
                for k, (src, dst) in enumerate(move_in(n, dest, slot)):
                    away = core == slot
                    if dest == slot:
                        @pl.when((y == dest) & (core == slot))
                        def _():
                            act(None, pltpu.make_async_copy(src, dst, in_recv.at[n, k, slot]))
                        away = away & (y != dest)

                    @pl.when(away)
                    def _():
                        act(remote(src, dst, in_send.at[n, k, dest], in_recv.at[n, k, slot], base + 2 * dest + y), None)

    def start(far, near):
        (far or near).start()

    def sent(far, near):
        if far is not None:
            far.wait_send()

    for n in range(len(segments)):
        each_move_in(n, start)

    def spread(value):
        return jnp.full((BLOCK, width), value, jnp.float32)

    for k in range(labels):
        damped = spread(damping[k]) * time_step / 2.0
        omega = spread(omega_zero[k])
        table[k] = time_step / spread(eps_inf[k])
        table[labels + k] = (1.0 - damped) / (1.0 + damped)
        table[2 * labels + k] = time_step * omega * omega / (1.0 + damped)
        table[3 * labels + k] = spread(delta_eps[k])

    cos_sin = []
    for axis in range(2):
        theta = spread(2.0 * math.pi) * spread(kpoint[axis].astype(jnp.float32)) / KGRID
        cos_sin.append((jnp.cos(theta), jnp.sin(theta)))
    (cos_x, sin_x), (cos_y, sin_y) = cos_sin
    turns = (((me >= gx - 4) & (core == 1), cos_x, sin_x), ((me < 4) & (core == 0), cos_x, -sin_x),
             (y == 0, cos_y, -sin_y), (y == 1, cos_y, sin_y))
    for i, (where, cosv, sinv) in enumerate(turns):
        phase[2 * i] = jnp.where(where, cosv, 1.0)
        phase[2 * i + 1] = jnp.where(where, sinv, 0.0)

    def wait_in(n, k):
        for slot in range(2):
            src, dst = move_in(n, 0, slot)[k]
            remote(src, dst, in_send.at[n, k, 0], in_recv.at[n, k, slot], base + lax.rem(q + 1, 4)).wait_recv()

    def move_out(c, k, i):
        lo, hi = outs[c]
        ref, out = ((e, e_out), (h, h_out))[k]
        src = ref.at[:, :, pl.ds(i * local, local), pl.ds(lo, hi - lo)]
        to = pl.multiple_of(y * half + (lo - LOW), BLOCK)
        return src, out.at[:, :, :, pl.ds(to, hi - lo)]

    def each_move_out(c, act):
        for k in range(2):
            for i in range(2):
                src, dst = move_out(c, k, i)
                here = (core == i) & (y == i)

                @pl.when(here)
                def _():
                    act(None, pltpu.make_async_copy(src, dst, ro.at[c, k, i]))

                @pl.when(jnp.logical_not(here))
                def _():
                    act(remote(src, dst, so.at[c, k, i], ro.at[c, k, y], base + 2 * core + i), None)

    def wait_out(c):
        for k in range(2):
            for other in range(2):
                src, dst = move_out(c, k, 0)
                remote(src, dst, so.at[c, k, 0], ro.at[c, k, other], base + lax.rem(q + 1, 4)).wait_recv()

    def halos(c, t, act):
        par = lax.rem(t, 2)

        def both(cut):
            kept = pl.ds(cut, sizes[c] - cut)
            for k, (send, recv, to) in enumerate(((se, re, left), (sh, rh, right))):
                act(remote(stages[c][k].at[:, :, kept], stages[c][2 + k].at[par, :, :, kept],
                           send.at[c], recv.at[c, par], to))

        if c:
            both(0)
        else:
            for k in range((ITERS - 1) // 4 + 1):
                @pl.when(lax.div(t - 1, 4) == k)
                def _():
                    both(BLOCK * k)

    def block_loop(c, t, body, unroll):
        count = sizes[c] // BLOCK
        first = 0
        if not c:
            first = (ITERS - 1) // 4
            for i in range(first):
                @pl.when(lax.div(t - 1, 4) <= i)
                def _():
                    body(i, 0)
        left_over = count - first
        lax.fori_loop(first, count, body, 0, unroll=unroll if left_over % unroll == 0 else 1)

    lane = lax.broadcasted_iota(jnp.int32, (BLOCK, width), 1)
    not_end = lane < width - 1
    not_start = lane > 0
    zero = jnp.zeros((BLOCK, width), jnp.float32)

    def rows_at(i):
        return pl.ds(i * BLOCK if isinstance(i, int) else pl.multiple_of(i * BLOCK, BLOCK), BLOCK)

    def next_z(f):
        return jnp.where(not_end, pltpu.roll(f, width - 1, 1), 0.0)

    def prev_z(f):
        return jnp.where(not_start, pltpu.roll(f, 1, 1), 0.0)

    @pl.loop(0, rows // BLOCK)
    def _(i):
        here = pl.ds(pl.multiple_of(i * BLOCK, BLOCK), BLOCK)
        for x in range(planes):
            for ri in range(2):
                for a in range(3):
                    pol[ri, a, x, here] = zero
                    cur[ri, a, x, here] = zero

    for x in range(planes):
        for which in range(4):
            coef[which, x, 0:BLOCK] = zero
        for ri in range(2):
            for a in range(3):
                e[ri, a, x, 0:BLOCK] = zero
                h[ri, a, x, 0:BLOCK] = zero

    def fill_coef(lo, hi):
        @pl.loop(0, (hi - lo) // BLOCK)
        def _(i):
            here = pl.ds(pl.multiple_of(lo + i * BLOCK, BLOCK), BLOCK)
            for x in range(planes):
                label = lab[x, here]
                masks = [label == k for k in range(labels)]
                for which in range(4):
                    picked = zero
                    for k, mask in enumerate(masks):
                        picked = picked + jnp.where(mask, table[which * labels + k], 0.0)
                    coef[which, x, here] = picked

    def turn_rows(ref, lo, hi, turn):
        @pl.loop(0, (hi - lo) // BLOCK)
        def _(i):
            here = pl.ds(pl.multiple_of(lo + i * BLOCK, BLOCK), BLOCK)
            for x in range(planes):
                for a in range(3):
                    re_new, im_new = turned(ref[0, a, x, here], ref[1, a, x, here], *turn)
                    ref[0, a, x, here] = re_new
                    ref[1, a, x, here] = im_new

    last = planes - 1

    def spots(c, t, i):
        at = BASE + starts[c] - t + i * BLOCK
        return [pl.ds(at + k, BLOCK) for k in (-1, 0, 1)] + [rows_at(i)]

    def prepare(c, t):
        stage_e, stage_h = stages[c][:2]

        def one(i, carry):
            down, here, up, to = spots(c, t, i)
            for ri in range(2):
                stage_e[ri, 0, to] = e[ri, 1, 0, here]
                stage_e[ri, 1, to] = e[ri, 2, 0, here]
                ex, ey, ez = [e[ri, a, last, here] for a in range(3)]
                hy = h[ri, 1, last, here] - time_step * ((next_z(ex) - ex) + ez)
                hz = h[ri, 2, last, here] + time_step * (ey + (e[ri, 0, last, up] - ex))
                h[ri, 1, last, here] = hy
                h[ri, 2, last, here] = hz
                stage_h[ri, 0, to] = hy
                stage_h[ri, 1, to] = hz
            return carry
        block_loop(c, t, one, UNROLL_P)
        halos(c, t, lambda copy: copy.start())

    def inner(c, t):
        def one(i, carry):
            down, here, up, to = spots(c, t, i)
            field = [[e[ri, a, 0, here] for a in range(3)] for ri in range(2)]
            for x in range(planes):
                if x < last:
                    later = [[e[ri, a, x + 1, here] for a in range(3)] for ri in range(2)]
                for ri in range(2):
                    ex, ey, ez = field[ri]
                    h[ri, 0, x, here] = h[ri, 0, x, here] - time_step * ((e[ri, 2, x, up] - ez) - (next_z(ey) - ey))
                    if x < last:
                        h[ri, 1, x, here] = h[ri, 1, x, here] - time_step * ((next_z(ex) - ex) - (later[ri][2] - ez))
                        h[ri, 2, x, here] = h[ri, 2, x, here] - time_step * ((later[ri][1] - ey) - (e[ri, 0, x, up] - ex))
                field = later
            return carry
        block_loop(c, t, one, UNROLL_H)

    def complete(c, t):
        ge = stages[c][2].at[lax.rem(t, 2)]

        def one(i, carry):
            down, here, up, to = spots(c, t, i)
            beyond = [turned(ge[0, a, to], ge[1, a, to], *turn_of(0)) for a in range(2)]
            for ri in range(2):
                h[ri, 1, last, here] = h[ri, 1, last, here] + time_step * beyond[1][ri]
                h[ri, 2, last, here] = h[ri, 2, last, here] - time_step * beyond[0][ri]
            return carry
        block_loop(c, t, one, UNROLL_P)

    def electric(c, t, order):
        gh = stages[c][3].at[lax.rem(t, 2)]

        def one(i, carry):
            down, here, up, to = spots(c, t, i)
            for x in order:
                if x:
                    prev_y, prev_zz = [[h[ri, a, x - 1, here] for ri in range(2)] for a in (1, 2)]
                else:
                    before = [turned(gh[0, a, to], gh[1, a, to], *turn_of(1)) for a in range(2)]
                    prev_y = [before[0][ri] + time_step * e[ri, 2, 0, here] for ri in range(2)]
                    prev_zz = [before[1][ri] - time_step * e[ri, 1, 0, here] for ri in range(2)]
                ce, ja, jb, de = [coef[k, x, here] for k in range(4)]
                for ri in range(2):
                    hx, hy, hz = [h[ri, a, x, here] for a in range(3)]
                    kx = (hz - h[ri, 2, x, down]) - (hy - prev_z(hy))
                    ky = (hx - prev_z(hx)) - (hz - prev_zz[ri])
                    kz = (hy - prev_y[ri]) - (hx - h[ri, 0, x, down])
                    for a, kurl in enumerate((kx, ky, kz)):
                        field, polar = e[ri, a, x, here], pol[ri, a, x, here]
                        current = ja * cur[ri, a, x, here] + jb * (de * field - polar)
                        cur[ri, a, x, here] = current
                        pol[ri, a, x, here] = polar + time_step * current
                        e[ri, a, x, here] = field + ce * (kurl - current)
            return carry
        block_loop(c, t, one, UNROLL_E)

    def advance(c, t):
        halos(c, t, lambda copy: copy.wait_recv())
        complete(c, t)
        electric(c, t, (0, last))
        halos(c, t, lambda copy: copy.wait_send())

        @pl.when(t < ITERS)
        def _():
            prepare(c, t + 1)
        electric(c, t, range(1, last))

        @pl.when(t < ITERS)
        def _():
            inner(c, t + 1)

        @pl.when(t == ITERS)
        def _():
            each_move_out(c, start)

    def arrive(c):
        mine = [n for n, (chunk, _) in enumerate(segments) if chunk == c]
        for n in mine:
            lo, hi = segments[n][1]
            for k, ref in enumerate((e, h)):
                wait_in(n, k)
                if hi <= LOW:
                    turn_rows(ref, lo, hi, turn_of(2))
                if lo >= LOW + half:
                    turn_rows(ref, lo, hi, turn_of(3))
        prepare(c, 1)
        inner(c, 1)
        for n in mine:
            wait_in(n, 2)
            fill_coef(*segments[n][1])

    waves = BEGIN[-1] + ITERS + 1

    @pl.loop(0, waves)
    def _(w):
        for c in range(CHUNKS):
            t = w - BEGIN[c]

            @pl.when((t >= 1) & (t <= ITERS))
            def _():
                advance(c, t)

        for c in range(CHUNKS):
            @pl.when(w == BEGIN[c])
            def _():
                arrive(c)

    for n in range(len(segments)):
        each_move_in(n, sent)
    for c in range(CHUNKS):
        each_move_out(c, sent)
        wait_out(c)


def shards(e_field, h_field, labels, kpoint, eps_inf, delta_eps, omega_zero, damping):
    local, total_rows, width = labels.shape
    half = total_rows // 2
    planes = 2 * local
    rows = half + LOW + GHOST
    state = (2, 3, local, total_rows, width)
    field = (2, 3, planes, rows, width)
    count = sum(len(p) for p in pieces_in(half))
    dma = pltpu.SemaphoreType.DMA
    anywhere = pl.BlockSpec(memory_space=pl.ANY)
    scalars = pl.BlockSpec(memory_space=pltpu.SMEM)
    halos = []
    for size in chunk_sizes(half):
        halos += [pltpu.VMEM((2, 2, size, width), jnp.float32)] * 2
        halos += [pltpu.VMEM((2, 2, 2, size, width), jnp.float32)] * 2
    return pl.pallas_call(
        kernel,
        out_shape=(jax.ShapeDtypeStruct(state, jnp.float32),) * 2,
        in_specs=[anywhere] * 3 + [scalars] * 5,
        out_specs=(anywhere, anywhere),
        scratch_shapes=[pltpu.VMEM(field, jnp.float32)] * 4
        + [pltpu.VMEM((4, planes, rows, width), jnp.float32), pltpu.VMEM((planes, rows, width), jnp.int32),
           pltpu.VMEM((4 * eps_inf.shape[0], BLOCK, width), jnp.float32), pltpu.VMEM((8, BLOCK, width), jnp.float32)]
        + halos
        + [dma((count, 3, 2)), dma((count, 3, 2)), dma((CHUNKS,)), dma((CHUNKS, 2)),
           dma((CHUNKS,)), dma((CHUNKS, 2)), dma((CHUNKS, 2, 2)), dma((CHUNKS, 2, 2))],
        compiler_params=pltpu.CompilerParams(collective_id=0, has_side_effects=True),
    )(e_field, h_field, labels, kpoint, eps_inf, delta_eps, omega_zero, damping)


def solution(mesh):
    placed = (
        P(None, None, ("kpt", "gx"), None, None),
        P(None, None, ("kpt", "gx"), None, None),
        P(("kpt", "gx"), None, None),
        P("kpt"),
        P(),
        P(),
        P(),
        P(),
    )
    return jax.shard_map(
        shards,
        mesh=mesh,
        in_specs=placed,
        out_specs=(
            P(None, None, ("kpt", "gx"), None, None),
            P(None, None, ("kpt", "gx"), None, None),
        ),
        check_vma=False,
    )
```
